64 devices in a mesh: data: 4 (over x, y), time: 16 (over z, core).
Axes of the slice: x: 2, y: 2, z: 8, core: 2. Of those that a mesh axis runs over, the one named last changes fastest.
The devices are a block of a 4x4x8 slice.
Arguments:
- x_init: float32 [4, 4096, 64], P('data'), parts along dimension 0
- w_in: bfloat16 [64, 1536], replicated
- w_out: bfloat16 [1536, 64], replicated
- mod_scale: bfloat16 [32, 1536], P('time')
- mod_shift: bfloat16 [32, 1536], P('time')
- step_size: float32 [32], P('time')
- noise_inc: float32 [32, 4, 4096, 64], P('time', 'data'), parts along dimension 1
Outputs:
- output: float32 [32, 4, 4096, 64], P('time', 'data'), parts along dimension 1
There are 4 independent parts. The reference program is written for one: setup_inputs(seed, part) draws one part's arguments, and reference() takes and returns one part's arrays. A program takes and returns all parts, laid end to end along the dimension named above; an argument that names none is the same for every part.
All inputs are finite; a program needn't handle non-finite values.
Results may differ from the reference program's by a relative error of at most 0.001.
Values are sent between devices in bfloat16 or wider.
A program may use at most 768 MiB of HBM per device.

```python
import jax
import jax.numpy as jnp
from jax import lax

BATCH = 1
TOKENS = 4096
CHANNELS = 64
HIDDEN = 1536
STEPS = 32
SWEEPS = 8


def setup_inputs(seed: int = 0, part: int = 0) -> dict:
    base_key = jax.random.key(seed)
    part_key = jax.random.fold_in(base_key, part)
    key_lat, key_noise = jax.random.split(part_key, 2)
    key_list = jax.random.split(jax.random.key(seed + 1), 6)
    w_first = jax.random.normal(key_list[0], (CHANNELS, HIDDEN), jnp.float32) * CHANNELS ** -0.5
    w_back = -(2.0 * CHANNELS / HIDDEN) * w_first.T + 0.5 * HIDDEN ** -0.5 * jax.random.normal(key_list[1], (HIDDEN, CHANNELS), jnp.float32)
    mod_scale = 0.2 * jax.random.normal(key_list[2], (STEPS, HIDDEN), jnp.float32)
    mod_shift = 0.5 * jax.random.normal(key_list[3], (STEPS, HIDDEN), jnp.float32)
    position = (jnp.arange(STEPS, dtype=jnp.float32) + 0.5) / STEPS
    tilt_coef = jax.random.uniform(key_list[4], (), jnp.float32, -1.0, 1.0)
    jitter = jax.random.uniform(key_list[5], (STEPS,), jnp.float32, 0.75, 1.25)
    step_size = (3.0 / STEPS) * jnp.exp(tilt_coef * (position - 0.5)) * jitter
    x_init = jax.random.normal(key_lat, (BATCH, TOKENS, CHANNELS), jnp.float32)
    noise_inc = 2.0 * STEPS ** -0.5 * jax.random.normal(key_noise, (STEPS, BATCH, TOKENS, CHANNELS), jnp.float32)
    return {
        "x_init": x_init,
        "w_in": w_first.astype(jnp.bfloat16),
        "w_out": w_back.astype(jnp.bfloat16),
        "mod_scale": mod_scale.astype(jnp.bfloat16),
        "mod_shift": mod_shift.astype(jnp.bfloat16),
        "step_size": step_size,
        "noise_inc": noise_inc,
    }


def drift_one(latents, scale_row, shift_row, step_row, w_in, w_out):
    flat_lat = latents.astype(jnp.bfloat16).reshape(BATCH * TOKENS, CHANNELS)
    pre_act = jnp.dot(flat_lat, w_in, preferred_element_type=jnp.float32)
    hidden = pre_act * (1.0 + scale_row.astype(jnp.float32)) + shift_row.astype(jnp.float32)
    gelu_out = jax.nn.gelu(hidden, approximate=True).astype(jnp.bfloat16)
    proj_out = jnp.dot(gelu_out, w_out, preferred_element_type=jnp.float32)
    return (step_row * proj_out).reshape(BATCH, TOKENS, CHANNELS)


def reference(x_init, w_in, w_out, mod_scale, mod_shift, step_size, noise_inc):
    def one_sweep(latents, unused):
        drifts = lax.map(lambda fields: drift_one(fields[0], fields[1], fields[2], fields[3], w_in, w_out), (latents, mod_scale, mod_shift, step_size))
        increments = drifts + noise_inc
        earlier = jnp.concatenate([jnp.zeros_like(increments[:1]), jnp.cumsum(increments[:-1], axis=0)], axis=0)
        return x_init[None] + earlier, None
    start_lat = jnp.broadcast_to(x_init[None], noise_inc.shape)
    final_lat, unused = lax.scan(one_sweep, start_lat, None, length=SWEEPS)
    return final_lat
```

```python
import functools
import math

import jax
import jax.numpy as jnp
from jax import lax
from jax.experimental import pallas as pl
from jax.experimental.pallas import tpu as pltpu
from jax.sharding import PartitionSpec as P

MESH = pl.DeviceIdType.MESH
SWEEPS = 8
HALF = SWEEPS // 2
LANES = 128
BLOCK = 256
GELU_A = 2.0 * math.sqrt(2.0 / math.pi)
GELU_B = 8.0 * math.sqrt(2.0 / math.pi) * 0.044715


def kernel(
    n_time, steps_own, chunks,
    x_hbm, w_in_ref, w_out_ref, mod_ref, step_ref, noise_hbm, out_hbm,
    latents, lat_bf, act, noise_buf, out_buf, x_own, x_full, mod_all, step_all, mod_cols,
    x_sem, full_sem, mod_send, mod_recv, step_send, step_recv, noise_send, noise_recv, out_send, out_recv,
):
    data, me = lax.axis_index("data"), lax.axis_index("time")
    steps = n_time * steps_own
    own = chunks * LANES
    channels = x_own.shape[0]
    hidden = w_in_ref.shape[0]
    half_hidden = hidden // 2
    group = HALF * LANES

    def lane_slice(device, chunk):
        return pl.ds(pl.multiple_of(device * own + chunk * LANES, LANES), LANES)

    def other(i):
        near = i // 2 + 1
        return lax.rem(me + jnp.where(lax.rem(i, 2) == 0, near, n_time - near), n_time)

    def remote(src, dst, send, recv, device):
        return pltpu.make_async_remote_copy(
            src_ref=src, dst_ref=dst, send_sem=send, recv_sem=recv,
            device_id=(data, device), device_id_type=MESH,
        )

    def mod_copy(device, slot):
        return remote(mod_ref, mod_all.at[slot], mod_send.at[device], mod_recv.at[slot], device)

    def step_copy(device, slot):
        return remote(step_ref, step_all.at[slot], step_send.at[device], step_recv.at[slot], device)

    def noise_copy(device, chunk, k, owner):
        return remote(
            noise_hbm.at[k, :, lane_slice(device, chunk)],
            noise_buf.at[chunk, owner * steps_own + k],
            noise_send.at[chunk, k, device],
            noise_recv.at[chunk, owner * steps_own + k],
            device,
        )

    def own_noise(chunk, k):
        return pltpu.make_async_copy(
            noise_hbm.at[k, :, lane_slice(me, chunk)],
            noise_buf.at[chunk, me * steps_own + k],
            noise_recv.at[chunk, me * steps_own + k],
        )

    def out_copy(chunk, j, source):
        return remote(
            out_buf.at[chunk, j],
            out_hbm.at[lax.rem(j, steps_own), :, lane_slice(source, chunk)],
            out_send.at[chunk, j],
            out_recv.at[chunk, lax.rem(j, steps_own), source],
            j // steps_own,
        )

    def own_out(chunk, j):
        return pltpu.make_async_copy(
            out_buf.at[chunk, j],
            out_hbm.at[lax.rem(j, steps_own), :, lane_slice(me, chunk)],
            out_recv.at[chunk, lax.rem(j, steps_own), me],
        )

    x_copy = pltpu.make_async_copy(x_hbm.at[:, pl.ds(pl.multiple_of(me * own, LANES), own)], x_own, x_sem)
    x_copy.start()

    barrier = pltpu.get_barrier_semaphore()

    @pl.loop(0, n_time - 1)
    def _(i):
        pl.semaphore_signal(barrier, inc=1, device_id=(data, other(i)), device_id_type=MESH)

    pl.semaphore_wait(barrier, n_time - 1)

    @pl.loop(0, n_time - 1)
    def _(i):
        mod_copy(other(i), me).start()
        step_copy(other(i), me).start()

    for chunk in range(chunks):
        for k in range(steps_own):
            own_noise(chunk, k).start()

            @pl.loop(0, n_time - 1)
            def _(i, chunk=chunk, k=k):
                noise_copy(other(i), chunk, k, me).start()

    @pl.when(me == 0)
    def _():
        full = pltpu.make_async_copy(x_hbm, x_full, full_sem)
        full.start()
        full.wait()
        pltpu.make_async_copy(x_full, out_hbm.at[0], full_sem).start()

    x_copy.wait()
    mod_all[me] = mod_ref[...]
    step_all[me] = step_ref[...]

    @pl.loop(0, n_time - 1)
    def _(i):
        mod_copy(me, other(i)).wait_recv()
        step_copy(me, other(i)).wait_recv()

    rows = mod_all[...].astype(jnp.float32).reshape(n_time * 8, half_hidden)
    is_scale = lax.rem(lax.broadcasted_iota(jnp.int32, rows.shape, 0), 8) < 2 * steps_own
    mod_cols[...] = (jnp.where(is_scale, 1.0 + rows, rows) * 0.5).T

    def column(block, j, kind):
        per_half = half_hidden // BLOCK
        lane = 8 * (j // steps_own) + 2 * (kind * steps_own + lax.rem(j, steps_own)) + block // per_half
        start = (block % per_half) * BLOCK
        index = jnp.full((BLOCK, LANES), lane, jnp.int32)
        return jnp.take_along_axis(mod_cols[start:start + BLOCK, :], index, axis=1)

    def drift(j, g):
        x_bf = lat_bf[:, g * group:(g + 1) * group]
        for block in range(hidden // BLOCK):
            pre = jnp.dot(w_in_ref[block * BLOCK:(block + 1) * BLOCK, :], x_bf, preferred_element_type=jnp.float32)
            scale = column(block, j, 0)
            shift = column(block, j, 1)
            for t in range(HALF):
                y = pre[:, t * LANES:(t + 1) * LANES] * scale + shift
                u = y * (y * y * GELU_B + GELU_A)
                a = y * jnp.tanh(u) + y
                act[g, block * BLOCK:(block + 1) * BLOCK, t * LANES:(t + 1) * LANES] = a.astype(jnp.bfloat16)
        return jnp.dot(w_out_ref[...], act[g], preferred_element_type=jnp.float32)

    def advance(chunk, j, g, proj, add):
        base = LANES + g * group
        for t in range(HALF):
            part = slice(base + t * LANES, base + (t + 1) * LANES)
            step = step_all[j // steps_own, pl.ds(lax.rem(j, steps_own), 1), :]
            latents[:, part] = latents[:, part] + (step * proj[:, t * LANES:(t + 1) * LANES] + add)

    def emit(chunk, j, slot):
        out_buf[chunk, j] = latents[:, slot * LANES:(slot + 1) * LANES]

    def send(chunk, j):
        @pl.when(j // steps_own == me)
        def _():
            own_out(chunk, j).start()

        @pl.when(j // steps_own != me)
        def _():
            out_copy(chunk, j, me).start()

    def wait_noise(chunk, j):
        @pl.when(j // steps_own == me)
        def _():
            own_noise(chunk, lax.rem(j, steps_own)).wait()

        @pl.when(j // steps_own != me)
        def _():
            noise_copy(me, chunk, lax.rem(j, steps_own), j // steps_own).wait_recv()

    @pl.loop(0, chunks)
    def _(chunk):
        start = x_own[:, pl.ds(pl.multiple_of(chunk * LANES, LANES), LANES)]
        for s in range(SWEEPS + 1):
            latents[:, s * LANES:(s + 1) * LANES] = start

        def one_step(j, groups, slot):
            wait_noise(chunk, j)
            lat_bf[...] = latents[:, :2 * group].astype(jnp.bfloat16)
            add = noise_buf[chunk, j]
            for g in groups:
                advance(chunk, j, g, drift(j, g), add)
            emit(chunk, j + 1, slot)

        @pl.loop(0, HALF)
        def _(j):
            @pl.when(j > 0)
            def _():
                send(chunk, j)

            one_step(j, (0,), HALF)

        reached = latents[:, HALF * LANES:(HALF + 1) * LANES]
        for s in range(HALF + 1, SWEEPS + 1):
            latents[:, s * LANES:(s + 1) * LANES] = reached

        @pl.loop(HALF, steps - 1 - HALF)
        def _(j):
            send(chunk, j)
            one_step(j, (0, 1), SWEEPS)

        @pl.loop(steps - 1 - HALF, steps - 1)
        def _(j):
            send(chunk, j)
            one_step(j, (1,), SWEEPS)

        send(chunk, steps - 1)

    @pl.loop(0, n_time - 1)
    def _(i):
        mod_copy(other(i), me).wait_send()
        step_copy(other(i), me).wait_send()
        for chunk in range(chunks):
            for k in range(steps_own):
                noise_copy(other(i), chunk, k, me).wait_send()

    for chunk in range(chunks):
        wait_noise(chunk, steps - 1)

        @pl.loop(1, steps)
        def _(j, chunk=chunk):
            @pl.when(j // steps_own != me)
            def _():
                out_copy(chunk, j, me).wait_send()

        for k in range(steps_own):
            @pl.loop(0, n_time)
            def _(source, chunk=chunk, k=k):
                j = me * steps_own + k

                @pl.when(j > 0)
                def _():
                    @pl.when(source == me)
                    def _():
                        own_out(chunk, j).wait()

                    @pl.when(source != me)
                    def _():
                        out_copy(chunk, j, source).wait_recv()

    @pl.when(me == 0)
    def _():
        pltpu.make_async_copy(x_full, out_hbm.at[0], full_sem).wait()


def solution(mesh):
    n_time = mesh.shape["time"]

    def body(x_init, w_in, w_out, mod_scale, mod_shift, step_size, noise_inc):
        steps_own, batch, tokens, channels = noise_inc.shape
        hidden = w_in.shape[1]
        own = tokens // n_time
        chunks = own // LANES
        steps = n_time * steps_own
        f32, bf16 = jnp.float32, jnp.bfloat16
        x_t = jnp.transpose(x_init, (0, 2, 1)).reshape(channels, tokens)
        noise_t = jnp.transpose(noise_inc, (0, 1, 3, 2)).reshape(steps_own, channels, tokens)
        mod = jnp.concatenate([mod_scale, mod_shift]).reshape(8, hidden // 2)
        step = jnp.broadcast_to(jnp.pad(step_size, (0, 8 - steps_own))[:, None], (8, LANES))
        vmem = pl.BlockSpec(memory_space=pltpu.VMEM)
        hbm = pl.BlockSpec(memory_space=pl.ANY)
        dma = pltpu.SemaphoreType.DMA
        out = pl.pallas_call(
            functools.partial(kernel, n_time, steps_own, chunks),
            out_shape=jax.ShapeDtypeStruct((steps_own, channels, tokens), f32),
            in_specs=[hbm, vmem, vmem, vmem, vmem, hbm],
            out_specs=hbm,
            scratch_shapes=[
                pltpu.VMEM((channels, (SWEEPS + 1) * LANES), f32),
                pltpu.VMEM((channels, SWEEPS * LANES), bf16),
                pltpu.VMEM((2, hidden, HALF * LANES), bf16),
                pltpu.VMEM((chunks, steps, channels, LANES), f32),
                pltpu.VMEM((chunks, steps, channels, LANES), f32),
                pltpu.VMEM((channels, own), f32),
                pltpu.VMEM((channels, tokens), f32),
                pltpu.VMEM((n_time, 8, hidden // 2), bf16),
                pltpu.VMEM((n_time, 8, LANES), f32),
                pltpu.VMEM((hidden // 2, n_time * 8), f32),
                dma(()), dma(()),
                dma((n_time,)), dma((n_time,)),
                dma((n_time,)), dma((n_time,)),
                dma((chunks, steps_own, n_time)), dma((chunks, steps)),
                dma((chunks, steps)), dma((chunks, steps_own, n_time)),
            ],
            compiler_params=pltpu.CompilerParams(
                collective_id=0, has_side_effects=True, vmem_limit_bytes=48 * 1024 * 1024
            ),
        )(x_t, w_in.T, w_out.T, mod, step, noise_t)
        return jnp.transpose(out.reshape(steps_own, batch, channels, tokens), (0, 1, 3, 2))

    return jax.shard_map(
        body,
        mesh=mesh,
        in_specs=(P("data"), P(), P(), P("time"), P("time"), P("time"), P("time", "data")),
        out_specs=P("time", "data"),
        check_vma=False,
    )
```
